256 devices in a mesh: grp: 4 (over x, y), row: 64 (over z, core).
Axes of the slice: x: 2, y: 2, z: 32, core: 2. Of those that a mesh axis runs over, the one named last changes fastest.
The devices are a block of a 4x8x32 slice.
Arguments:
- members_in: bfloat16 [2048, 4096], P(('grp', 'row')), parts along dimension 0, may hold values from -6 to 6
- gate_up: bfloat16 [4096, 2, 14336], P(None, None, 'row'), may hold values from -0.09375 to 0.09375
- down_weight: bfloat16 [14336, 4096], P('row'), may hold values from -0.046875 to 0.046875
- factor_in: bfloat16 [2048, 4, 4096], P('grp', None, 'row'), parts along dimension 0, may hold values from -0.09375 to 0.09375
- factor_out: bfloat16 [2048, 4, 2, 14336], P('grp', None, None, 'row'), parts along dimension 0, may hold values from -6 to 6
- target: float32 [2048, 4096], P(('grp', 'row')), parts along dimension 0, may hold values from -6 to 6
Outputs:
- outputs: bfloat16 [2048, 4096], P(('grp', 'row')), parts along dimension 0
- fitness: float32 [2048], P(('grp', 'row')), parts along dimension 0
- update: float32 [16384, 2, 14336], P('grp', None, 'row'), parts along dimension 0
The draws below stay inside these ranges and needn't reach their ends.
There are 4 independent parts, one for each index of `grp`. The reference program is written for one: setup_inputs(seed, part) draws one part's arguments, and reference() takes and returns one part's arrays. A program takes and returns all parts, laid end to end along the dimension named above; an argument that names none is the same for every part. Nothing has to cross between parts.
All inputs are finite; a program needn't handle non-finite values.
Results may differ from the reference program's by a relative error of at most 0.0049.
Values may be sent and summed in bfloat16 or wider, within the bound.
No kernel may reach another device: no remote copies, remote signals or barrier semaphores. Data moves between devices by JAX's collectives and lax.ppermute only.
A program may use at most 128 MiB of HBM per device.

```python
import math
import jax
import jax.numpy as jnp
from jax import lax

D = 4096
FF = 14336
RANK = 4
MEMBERS = 512


def draw_target(key, part):
    base_key = jax.random.fold_in(key, 7001)
    first, second = jax.random.split(base_key)
    places = jnp.arange(MEMBERS).astype(jnp.float32) / max(MEMBERS - 1, 1)
    jitter = jnp.exp(jax.random.uniform(second, (MEMBERS,), jnp.float32, -0.22, 0.22))
    values = jnp.clip(jax.random.normal(first, (MEMBERS, D), jnp.float32), -3.0, 3.0)
    ramp = 0.5 + places
    return (values * (ramp * jitter)[:, None]).astype(jnp.float32)


def block_levels(rng, shape, cuts, low, high):
    level = 1.0
    for position, shards_of in cuts:
        heights = jax.random.uniform(jax.random.fold_in(jax.random.fold_in(rng, 6), position), (shards_of,), jnp.float32, low / len(cuts), high / len(cuts))
        level = level * jnp.repeat(jnp.exp(heights), shape[position] // shards_of).reshape((-1,) + (1,) * (len(shape) - 1 - position))
    return level


def gaussian(rng, extent, deviation, limit, cuts=(), kind=jnp.bfloat16):
    result = jax.random.normal(rng, extent, jnp.float32) * deviation
    if len(cuts) > 0:
        result = block_levels(rng, extent, cuts, -0.22, 0.18) * result
    return jnp.clip(result, min=-limit, max=limit).astype(kind)


def setup_inputs(seed: int = 0, part: int = 0) -> dict:
    key_list = jax.random.split(jax.random.key(seed), 7)
    own_keys = jax.random.split(jax.random.fold_in(key_list[6], part), 7)
    return {
        "members_in": gaussian(own_keys[0], (MEMBERS, D), 1.0, 6.0, ((0, 64),)),
        "gate_up": gaussian(key_list[1], (D, 2, FF), D ** -0.5, 0.09375, ((2, 64),)),
        "down_weight": gaussian(key_list[2], (FF, D), FF ** -0.5, 0.046875, ((0, 64),)),
        "factor_in": gaussian(own_keys[3], (MEMBERS, RANK, D), D ** -0.5, 0.09375, ((2, 64),)),
        "factor_out": gaussian(own_keys[4], (MEMBERS, RANK, 2, FF), 1.0, 6.0, ((3, 64),)),
        "target": draw_target(jax.random.fold_in(jax.random.fold_in(key_list[6], part), 71), part),
    }


noise_scale = 0.5

def reference(members_in, gate_up, down_weight, factor_in, factor_out, target):
    highest = lax.Precision.HIGHEST
    inputs = members_in.astype(jnp.float32)
    factor_a = factor_in.astype(jnp.float32)
    factor_b = factor_out.astype(jnp.float32)
    projected = jnp.einsum('md,mrd->mr', inputs, factor_a, precision=highest)
    stacked = jnp.dot(inputs, gate_up.reshape(D, 2 * FF).astype(jnp.float32), precision=highest)
    stacked = stacked.reshape(MEMBERS, 2, FF)
    noise = jnp.einsum('mr,mrkf->mkf', projected, factor_b, precision=highest)
    stacked = stacked + noise * (noise_scale / math.sqrt(RANK))
    hidden = (jax.nn.silu(stacked[:, 0]) * stacked[:, 1]).astype(jnp.bfloat16)
    sums = jnp.dot(hidden.astype(jnp.float32), down_weight.astype(jnp.float32), precision=highest)
    losses = lax.optimization_barrier(jnp.mean((sums - target) ** 2, axis=1))
    average = jnp.mean(losses)
    spread = jnp.mean((losses - average) ** 2)
    fitness = (average - losses) / jnp.sqrt(spread + 1e-06)
    scaled = (fitness[:, None, None, None] * factor_b).astype(jnp.bfloat16)
    update = lax.dot_general(factor_a, scaled.astype(jnp.float32), (((0, 1), (0, 1)), ((), ())), precision=highest)
    update = update * math.sqrt(D / (MEMBERS * RANK))
    return (sums.astype(jnp.bfloat16), fitness, update)
```

```python
import functools
import math

import jax
import jax.numpy as jnp
from jax import lax
from jax.sharding import Mesh
from jax.sharding import PartitionSpec as P

ROW = ("z", "c")
GRP_ROW = ("grp", "z", "c")

noise_scale = 0.5
HIGHEST = lax.Precision.HIGHEST


def shifts(n, first, second):
    return [(2 * i, 2 * ((i + first) % n)) for i in range(n)] + [
        (2 * i + 1, 2 * ((i + second) % n) + 1) for i in range(n)
    ]


def swap_halves(value):
    return lax.all_to_all(
        jnp.broadcast_to(value[None], (2, *value.shape)), "c", 0, 0, tiled=True
    )


def body(members_in, gate_up, down_weight, factor_in, factor_out, target):
    own_rows = members_in.shape[0]
    width = gate_up.shape[0]
    local_units = gate_up.shape[2]
    members = factor_in.shape[0]
    rank = factor_in.shape[1]
    local_width = factor_in.shape[2]
    chips = lax.axis_size("z")
    arc = chips // 2
    pair = 2 * own_rows
    z = lax.axis_index("z")
    c = lax.axis_index("c")

    all_factor_in = lax.all_gather(factor_in, ROW, axis=2, tiled=True)

    place = jnp.arange(members)
    step = place // pair
    source = jnp.where(step < arc, z - 1 - step, z + step - arc)
    source = jnp.where(source < 0, source + chips, source)
    source = jnp.where(source >= chips, source - chips, source)
    order = source * pair + place % pair
    chosen = jnp.arange(members)[:, None] == order[None, :]
    chosen_low = chosen.astype(jnp.bfloat16)
    chosen_full = chosen.astype(jnp.float32)
    near_out = jnp.einsum(
        "mrkf,mn->rkfn", factor_out, chosen_low, preferred_element_type=jnp.bfloat16
    )
    near_in = jnp.einsum(
        "mrd,mn->rdn", factor_in, chosen_low, preferred_element_type=jnp.bfloat16
    )

    chip_x = lax.all_gather(members_in, "c", axis=0, tiled=True)
    block = lax.ppermute(chip_x, ROW, shifts(chips, 1, 0))
    blocks = [block]
    onward = shifts(chips, 1, -1)
    for _ in range(arc - 1):
        block = lax.ppermute(block, ROW, onward)
        blocks.append(block)
    near_x = swap_halves(jnp.concatenate(blocks, axis=0)).reshape(members, width)

    x_columns = lax.dynamic_slice_in_dim(
        near_x, (2 * z + c) * local_width, local_width, 1
    )
    partial_proj = jnp.sum(
        near_in.astype(jnp.float32) * x_columns.astype(jnp.float32).T[None], axis=1
    )
    partial_proj = jnp.dot(partial_proj, chosen_full.T, precision=HIGHEST)
    projected = jnp.sum(lax.all_gather(lax.psum(partial_proj, "z"), "c", axis=0), axis=0)
    near_projected = jnp.dot(projected, chosen_full, precision=HIGHEST)

    stacked = lax.dot_general(
        gate_up, near_x, (((0,), (1,)), ((), ())), preferred_element_type=jnp.float32
    )
    noise = jnp.sum(near_projected[:, None, None, :] * near_out.astype(jnp.float32), axis=0)
    stacked = stacked + noise * (noise_scale / math.sqrt(rank))
    hidden = (jax.nn.silu(stacked[0]) * stacked[1]).astype(jnp.bfloat16)
    partial = lax.dot_general(
        hidden, down_weight, (((0,), (0,)), ((), ())), preferred_element_type=jnp.float32
    )

    partial = partial.reshape(2, members // 2, width)
    halves = lax.all_to_all(partial.astype(jnp.bfloat16), "c", 0, 0, tiled=True)
    mine = lax.dynamic_index_in_dim(partial, c, 0, keepdims=False)
    other = lax.dynamic_index_in_dim(halves, 1 - c, 0, keepdims=False)
    side = (mine + other.astype(jnp.float32)).reshape(arc, pair, width)
    back = shifts(chips, -1, 1)
    total = side[arc - 1]
    for k in range(arc - 2, -1, -1):
        kind = jnp.bfloat16 if arc - 1 - k <= arc // 2 else jnp.float32
        total = lax.ppermute(total.astype(kind), ROW, back).astype(jnp.float32) + side[k]
    total = total.reshape(2, own_rows, width)
    crossing = lax.dynamic_index_in_dim(total, 1 - c, 0, keepdims=False)
    staying = lax.dynamic_index_in_dim(total, c, 0, keepdims=False)
    cross = [(2 * i, 2 * ((i - 1) % chips) + 1) for i in range(chips)] + [
        (2 * i + 1, 2 * i) for i in range(chips)
    ]
    sums = lax.ppermute(crossing, ROW, cross) + lax.ppermute(
        staying, ROW, shifts(chips, -1, 0)
    )

    own_losses = jnp.mean((sums - target) ** 2, axis=1)
    chip_losses = lax.all_gather(own_losses, "c", axis=0, tiled=True)
    spot = jnp.arange(members) // pair == z
    losses = lax.psum(
        jnp.where(spot, jnp.tile(chip_losses, chips), jnp.zeros((), jnp.float32)), "z"
    )
    average = jnp.mean(losses)
    spread = jnp.mean((losses - average) ** 2)
    all_fitness = (average - losses) / jnp.sqrt(spread + 1e-06)
    own_fitness = lax.dynamic_slice_in_dim(
        all_fitness, (2 * z + c) * own_rows, own_rows, 0
    )
    scaled = (all_fitness[:, None, None, None] * factor_out).astype(jnp.bfloat16)
    update = lax.dot_general(
        all_factor_in,
        scaled,
        (((0, 1), (0, 1)), ((), ())),
        preferred_element_type=jnp.float32,
    )
    update = update * math.sqrt(width / (members * rank))
    return (sums.astype(jnp.bfloat16), own_fitness, update)


def solution(mesh):
    groups = mesh.shape["grp"]
    finer = Mesh(mesh.devices.reshape(groups, -1, 2), ("grp", "z", "c"))
    return jax.shard_map(
        body,
        mesh=finer,
        in_specs=(
            P(GRP_ROW, None),
            P(None, None, ROW),
            P(ROW, None),
            P("grp", None, ROW),
            P("grp", None, None, ROW),
            P(GRP_ROW, None),
        ),
        out_specs=(P(GRP_ROW, None), P(GRP_ROW), P("grp", None, ROW)),
        check_vma=False,
    )
```
